32 devices in a mesh: grp: 2 (over y), row: 16 (over z, x, core).
Axes of the slice: x: 2, y: 2, z: 4, core: 2. Of those that a mesh axis runs over, the one named last changes fastest.
Arguments:
- diag_blocks: float32 [8192, 512], P('row'), may hold values from -0.6 to 2.6
- lower_coupling: float32 [8192, 64], P('row'), may hold values from -0.3125 to 0.3125
- upper_coupling: float32 [8192, 64], P('row'), may hold values from -0.3125 to 0.3125
- right_sides: float32 [8192, 1024], P('row', 'grp'), parts along dimension 1, may hold values from -108 to 108
Outputs:
- solution: float32 [8192, 1024], P('row', 'grp'), parts along dimension 1
- res_norms: float32 [8, 1024], P(None, 'grp'), parts along dimension 1
The draws below stay inside these ranges and needn't reach their ends.
There are 2 independent parts, one for each index of `grp`. The reference program is written for one: setup_inputs(seed, part) draws one part's arguments, and reference() takes and returns one part's arrays. A program takes and returns all parts, laid end to end along the dimension named above; an argument that names none is the same for every part. Nothing has to cross between parts.
All inputs are finite; a program needn't handle non-finite values.
Results may differ from the reference program's by a relative error of at most 0.0001.
Values sent between devices are 32-bit elements; how exact they have to be, the bound alone decides.
A program may use at most 64 MiB of HBM per device.

```python
import math
import jax
import jax.numpy as jnp
from jax import lax

B = 512
W = 64
C = 512
SWEEPS = 8
N = 8192
N_ROW = 16


def draw_diag_blocks(key, part):
    first, second = jax.random.split(jax.random.fold_in(key, 31), 2)
    noise = jnp.clip(jax.random.normal(first, (N, B), jnp.float32), -4.0, 4.0)
    noise = noise * (0.8 / math.sqrt(B))
    pivots = jax.random.uniform(second, (N, 1), jnp.float32, 1.0, 2.0)
    local_rows = (jnp.arange(N, dtype=jnp.int32) % B)[:, None]
    columns = jnp.arange(B, dtype=jnp.int32)[None, :]
    marker = (local_rows == columns).astype(jnp.float32)
    return (noise + marker * pivots).astype(jnp.float32)


def draw_right_sides(key, part):
    first, second, third = jax.random.split(jax.random.fold_in(key, 47), 3)
    base = jnp.clip(jax.random.normal(first, (N, C), jnp.float32), -4.0, 4.0)
    trend = jnp.exp(math.log(3.0) * jnp.arange(N, dtype=jnp.float32) / N)[:, None]
    row_scale = jnp.exp(jax.random.uniform(second, (N, 1), jnp.float32, math.log(0.3), math.log(3.0)))
    col_scale = jnp.exp(jax.random.uniform(third, (1, C), jnp.float32, math.log(0.3), math.log(3.0)))
    return (base * trend * row_scale * col_scale).astype(jnp.float32)


def block_levels(key, shape, shards, least, largest):
    gain = 1.0
    for position, parts in shards:
        draws = jax.random.uniform(jax.random.fold_in(jax.random.fold_in(key, 6), position), (parts,), jnp.float32, least / len(shards), largest / len(shards))
        gain = gain * jnp.repeat(jnp.exp(draws), shape[position] // parts).reshape((-1,) + (1,) * (len(shape) - 1 - position))
    return gain


def bell_draw(rng, extent, spread, most, shards=(), held_as=jnp.bfloat16):
    drawn = jax.random.normal(rng, extent, jnp.float32) * spread
    if len(shards) > 0:
        drawn = block_levels(rng, extent, shards, -0.22, 0.18) * drawn
    return jnp.clip(drawn, min=-most, max=most).astype(held_as)


def setup_inputs(seed: int = 0, part: int = 0) -> dict:
    seeds = jax.random.split(jax.random.key(seed), 5)
    part_keys = jax.random.split(jax.random.fold_in(seeds[4], part), 5)
    diag_blocks = draw_diag_blocks(jax.random.fold_in(seeds[4], 71), part)
    lower_coupling = bell_draw(seeds[1], (N, W), (6 * W) ** -0.5, 0.3125, ((0, 16),), jnp.float32)
    upper_coupling = bell_draw(seeds[2], (N, W), (6 * W) ** -0.5, 0.3125, ((0, 16),), jnp.float32)
    right_sides = draw_right_sides(jax.random.fold_in(jax.random.fold_in(seeds[4], part), 71), part)
    return dict(diag_blocks=diag_blocks, lower_coupling=lower_coupling, upper_coupling=upper_coupling, right_sides=right_sides)


def reference(diag_blocks, lower_coupling, upper_coupling, right_sides):
    blocks = diag_blocks.reshape(N_ROW, B, B)
    lower_blocks = lower_coupling.reshape(N_ROW, B, W)
    upper_blocks = upper_coupling.reshape(N_ROW, B, W)
    sources = right_sides.reshape(N_ROW, B, C)
    pivots = jnp.diagonal(blocks, axis1=1, axis2=2)[:, :, None]
    solution = jnp.zeros((N_ROW, B, C), jnp.float32)
    norm_list = []
    for sweep_index in range(SWEEPS):
        before_rims = jnp.concatenate([jnp.zeros((1, W, C), jnp.float32), solution[:-1, B - W:]], 0)
        after_rims = jnp.concatenate([solution[1:, :W], jnp.zeros((1, W, C), jnp.float32)], 0)
        images = jnp.einsum('kij,kjc->kic', blocks, solution, precision=lax.Precision.HIGHEST)
        images = images + jnp.einsum('kiw,kwc->kic', lower_blocks, before_rims, precision=lax.Precision.HIGHEST)
        images = images + jnp.einsum('kiw,kwc->kic', upper_blocks, after_rims, precision=lax.Precision.HIGHEST)
        residual = sources - images
        norm_list.append(jnp.sqrt(lax.optimization_barrier(jnp.sum(residual * residual, axis=(0, 1)))))
        solution = solution + residual / pivots
    return (solution.reshape(N_ROW * B, C), jnp.stack(norm_list))
```

```python
import functools

import jax
import jax.numpy as jnp
from jax import lax
from jax.experimental import pallas as pl
from jax.experimental.pallas import tpu as pltpu
from jax.sharding import PartitionSpec as P

SWEEPS = 8
LANES = 128


def split(value):
    high = value.astype(jnp.bfloat16)
    low = (value - high.astype(jnp.float32)).astype(jnp.bfloat16)
    return high, low


def dot(left, right):
    return jnp.dot(left, right, preferred_element_type=jnp.float32)


def kernel(
    n, d_hbm, l_hbm, u_hbm, b_hbm, x_out, norm_out,
    dv, lv, uv, xs, a_hi, a_lo, c_hi, c_lo, inv, acc, rhs, halo,
    send, recv, part, parts, load_sem, send_sem, recv_sem, psend, precv, out_sem,
):
    me = lax.axis_index("row")
    rows, cols = xs.shape
    width = lv.shape[1]
    groups = cols // LANES
    has = (me > 0, me < n - 1)
    last = rows - width

    loads = [pltpu.make_async_copy(d_hbm, dv, load_sem.at[0]),
             pltpu.make_async_copy(b_hbm, xs, load_sem.at[1]),
             pltpu.make_async_copy(l_hbm, lv, load_sem.at[2]),
             pltpu.make_async_copy(u_hbm, uv, load_sem.at[3])]
    for load in loads:
        load.start()

    barrier = pltpu.get_barrier_semaphore()

    def greet(o, carry):
        pl.semaphore_signal(barrier, inc=1, device_id={"row": lax.rem(me + o, n)})
        return carry

    lax.fori_loop(1, n, greet, 0)

    for side in range(2):
        @pl.when(jnp.logical_not(has[side]))
        def _():
            recv[:, side] = jnp.zeros_like(recv[:, side])

    def copy(s, side, g):
        target = me + 1 if side == 0 else me - 1
        return pltpu.make_async_remote_copy(
            src_ref=send.at[s, side, g], dst_ref=recv.at[s, side, g],
            send_sem=send_sem.at[s, side, g], recv_sem=recv_sem.at[s, side, g],
            device_id={"row": target})

    def ship(s, g):
        for side in range(2):
            @pl.when(has[1 - side])
            def _():
                copy(s, side, g).start()

    def keep(r, top, g):
        size = r.shape[0]
        d = r * inv[top:top + size]
        high, low = split(d)
        rhs[top:top + size, :LANES] = high
        rhs[top:top + size, LANES:] = low
        return d, jnp.sum(r * r, axis=0, keepdims=True)

    def advance(g):
        both = dot(a_hi[...], rhs[...])
        acc[g] = both[:, :LANES] + both[:, LANES:] + dot(a_lo[...], rhs[:, :LANES])

    def span(g):
        return slice(g * LANES, (g + 1) * LANES)

    loads[0].wait()
    for m in range(rows // LANES):
        block = dv[m * LANES:(m + 1) * LANES, m * LANES:(m + 1) * LANES]
        eye = (lax.broadcasted_iota(jnp.int32, block.shape, 0)
               == lax.broadcasted_iota(jnp.int32, block.shape, 1))
        pivot = jnp.sum(jnp.where(eye, block, 0.0), axis=1, keepdims=True)
        inv[m * LANES:(m + 1) * LANES] = jnp.broadcast_to(1.0 / pivot, block.shape)
    loads[1].wait()
    for g in range(groups):
        send[0, 1, g] = xs[:width, span(g)] * inv[:width]
        send[0, 0, g] = xs[last:, span(g)] * inv[last:]
    pl.semaphore_wait(barrier, n - 1)
    for g in range(groups):
        ship(0, g)

    for m in range(rows // LANES):
        block = dv[m * LANES:(m + 1) * LANES]
        eye = (lax.broadcasted_iota(jnp.int32, block.shape, 0) + m * LANES
               == lax.broadcasted_iota(jnp.int32, block.shape, 1))
        a_hi[m * LANES:(m + 1) * LANES], a_lo[m * LANES:(m + 1) * LANES] = split(
            jnp.where(eye, 0.0, -block))
    loads[2].wait()
    loads[3].wait()
    c_hi[...], c_lo[...] = split(-jnp.concatenate([lv[...], uv[...]], axis=1))

    for g in range(groups):
        d, sums = keep(xs[:, span(g)], 0, g)
        part[0, g:g + 1] = sums
        xs[:, span(g)] = d
        advance(g)

    def sweep(s, final):
        for g in range(groups):
            for side in range(2):
                @pl.when(has[side])
                def _():
                    copy(s - 1, side, g).wait_recv()
            for side in range(2):
                high, low = split(recv[s - 1, side, g])
                halo[side * width:(side + 1) * width, :LANES] = high
                halo[side * width:(side + 1) * width, LANES:] = low

            def rest(top, size):
                both = dot(c_hi[top:top + size], halo[...])
                cross = dot(c_lo[top:top + size], halo[:, :LANES])
                return acc[g, top:top + size] + (both[:, :LANES] + both[:, LANES:] + cross)

            total = jnp.zeros((1, LANES), jnp.float32)
            for top, size in ((0, width), (last, width), (width, last - width)):
                d, sums = keep(rest(top, size), top, g)
                total = total + sums
                if size == width and not final:
                    send[s, 1 if top == 0 else 0, g] = d
                    if top == last:
                        ship(s, g)
                xs[top:top + size, span(g)] += d
            part[s, g:g + 1] = total
            if final:
                pltpu.make_async_copy(
                    xs.at[:, span(g)], x_out.at[:, span(g)], out_sem.at[g]).start()
            else:
                advance(g)

    def body(s, carry):
        sweep(s, False)
        return carry

    def spread(lane, start):
        lo, hi = ((0, SWEEPS - 1), (SWEEPS - 1, SWEEPS))[lane]

        def one(o, carry):
            peer = pltpu.make_async_remote_copy(
                src_ref=part.at[lo:hi], dst_ref=parts.at[me, lo:hi],
                send_sem=psend.at[lane, o], recv_sem=precv.at[lane, o],
                device_id={"row": lax.rem(me + o, n)})
            if start:
                peer.start()
            else:
                peer.wait_send()
            return carry

        lax.fori_loop(1, n, one, 0)

    def collect(lane):
        lo, hi = ((0, SWEEPS - 1), (SWEEPS - 1, SWEEPS))[lane]

        def one(o, carry):
            source = lax.rem(me + n - o, n)
            pltpu.make_async_remote_copy(
                src_ref=part.at[lo:hi], dst_ref=parts.at[source, lo:hi],
                send_sem=psend.at[lane, o], recv_sem=precv.at[lane, o],
                device_id={"row": lax.rem(me + o, n)}).wait_recv()
            return carry

        lax.fori_loop(1, n, one, 0)

    lax.fori_loop(1, SWEEPS - 1, body, 0)
    spread(0, True)
    sweep(SWEEPS - 1, True)
    spread(1, True)
    parts[me] = part[...]

    def drain(s, carry):
        for side in range(2):
            for g in range(groups):
                @pl.when(has[1 - side])
                def _():
                    copy(s, side, g).wait_send()
        return carry

    lax.fori_loop(0, SWEEPS - 1, drain, 0)
    collect(0)
    collect(1)
    norms = jnp.sqrt(lax.fori_loop(0, n, lambda j, t: t + parts[j], jnp.zeros(part.shape, jnp.float32)))
    for s in range(SWEEPS):
        for g in range(groups):
            norm_out[s:s + 1, span(g)] = norms[s, g:g + 1]
    spread(0, False)
    spread(1, False)
    for g in range(groups):
        pltpu.make_async_copy(xs.at[:, span(g)], x_out.at[:, span(g)], out_sem.at[g]).wait()


def local(n, diag_blocks, lower_coupling, upper_coupling, right_sides):
    rows, cols = right_sides.shape
    width = lower_coupling.shape[1]
    groups = cols // LANES
    f32, bf16 = jnp.float32, jnp.bfloat16
    return pl.pallas_call(
        functools.partial(kernel, n),
        out_shape=(jax.ShapeDtypeStruct((rows, cols), f32), jax.ShapeDtypeStruct((SWEEPS, cols), f32)),
        in_specs=[pl.BlockSpec(memory_space=pl.ANY)] * 4,
        out_specs=(pl.BlockSpec(memory_space=pl.ANY), pl.BlockSpec(memory_space=pltpu.VMEM)),
        scratch_shapes=[
            pltpu.VMEM((rows, rows), f32),
            pltpu.VMEM((rows, width), f32),
            pltpu.VMEM((rows, width), f32),
            pltpu.VMEM((rows, cols), f32),
            pltpu.VMEM((rows, rows), bf16),
            pltpu.VMEM((rows, rows), bf16),
            pltpu.VMEM((rows, 2 * width), bf16),
            pltpu.VMEM((rows, 2 * width), bf16),
            pltpu.VMEM((rows, LANES), f32),
            pltpu.VMEM((groups, rows, LANES), f32),
            pltpu.VMEM((rows, 2 * LANES), bf16),
            pltpu.VMEM((2 * width, 2 * LANES), bf16),
            pltpu.VMEM((SWEEPS - 1, 2, groups, width, LANES), f32),
            pltpu.VMEM((SWEEPS - 1, 2, groups, width, LANES), f32),
            pltpu.VMEM((SWEEPS, groups, LANES), f32),
            pltpu.VMEM((n, SWEEPS, groups, LANES), f32),
            pltpu.SemaphoreType.DMA((4,)),
            pltpu.SemaphoreType.DMA((SWEEPS - 1, 2, groups)),
            pltpu.SemaphoreType.DMA((SWEEPS - 1, 2, groups)),
            pltpu.SemaphoreType.DMA((2, n)),
            pltpu.SemaphoreType.DMA((2, n)),
            pltpu.SemaphoreType.DMA((groups,)),
        ],
        compiler_params=pltpu.CompilerParams(collective_id=0, has_side_effects=True),
    )(diag_blocks, lower_coupling, upper_coupling, right_sides)


def solution(mesh):
    return jax.shard_map(
        functools.partial(local, mesh.shape["row"]),
        mesh=mesh,
        in_specs=(P("row", None), P("row", None), P("row", None), P("row", "grp")),
        out_specs=(P("row", "grp"), P(None, "grp")),
        check_vma=False,
    )
```

```python
import functools

import jax
import jax.numpy as jnp
from jax import lax
from jax.experimental import pallas as pl
from jax.experimental.pallas import tpu as pltpu
from jax.sharding import PartitionSpec as P

SWEEPS = 8
LANES = 128


def split(value):
    high = value.astype(jnp.bfloat16)
    low = (value - high.astype(jnp.float32)).astype(jnp.bfloat16)
    return high, low


def dot(left, right):
    return jnp.dot(left, right, preferred_element_type=jnp.float32)


def kernel(
    n, d_hbm, l_hbm, u_hbm, b_hbm, x_out, norm_out,
    dv, lv, uv, xs, a_hi, a_lo, c_hi, c_lo, inv, acc, rhs, halo,
    send, recv, part, nears, fars, lates, load_sem, send_sem, recv_sem, psend, precv, out_sem,
):
    me = lax.axis_index("row")
    rows, cols = xs.shape
    width = lv.shape[0]
    groups = cols // LANES
    has = (me > 0, me < n - 1)
    last = rows - width

    loads = [pltpu.make_async_copy(d_hbm, dv, load_sem.at[0]),
             pltpu.make_async_copy(b_hbm, xs, load_sem.at[1]),
             pltpu.make_async_copy(l_hbm, lv, load_sem.at[2]),
             pltpu.make_async_copy(u_hbm, uv, load_sem.at[3])]
    for load in loads:
        load.start()

    barrier = pltpu.get_barrier_semaphore()

    def greet(o, carry):
        pl.semaphore_signal(barrier, inc=1, device_id={"row": lax.rem(me + o, n)})
        return carry

    lax.fori_loop(1, n, greet, 0)

    for side in range(2):
        @pl.when(jnp.logical_not(has[side]))
        def _():
            recv[:, side] = jnp.zeros_like(recv[:, side])

    def copy(s, side, g):
        target = me + 1 if side == 0 else me - 1
        return pltpu.make_async_remote_copy(
            src_ref=send.at[s, side, g], dst_ref=recv.at[s, side, g],
            send_sem=send_sem.at[s, side, g], recv_sem=recv_sem.at[s, side, g],
            device_id={"row": target})

    def ship(s, g):
        for side in range(2):
            @pl.when(has[1 - side])
            def _():
                copy(s, side, g).start()

    def keep(r, top, g):
        size = r.shape[0]
        d = r * inv[top:top + size]
        high, low = split(d)
        rhs[top:top + size, :LANES] = high
        rhs[top:top + size, LANES:] = low
        return d, jnp.sum(r * r, axis=0, keepdims=True)

    def advance(g):
        both = dot(a_hi[...], rhs[...])
        acc[g] = both[:, :LANES] + both[:, LANES:] + dot(a_lo[...], rhs[:, :LANES])

    def span(g):
        return slice(g * LANES, (g + 1) * LANES)

    loads[0].wait()
    for m in range(rows // LANES):
        block = dv[m * LANES:(m + 1) * LANES, m * LANES:(m + 1) * LANES]
        eye = (lax.broadcasted_iota(jnp.int32, block.shape, 0)
               == lax.broadcasted_iota(jnp.int32, block.shape, 1))
        pivot = jnp.sum(jnp.where(eye, block, 0.0), axis=1, keepdims=True)
        inv[m * LANES:(m + 1) * LANES] = jnp.broadcast_to(1.0 / pivot, block.shape)
    loads[1].wait()
    for g in range(groups):
        send[0, 1, g] = xs[:width, span(g)] * inv[:width]
        send[0, 0, g] = xs[last:, span(g)] * inv[last:]
    pl.semaphore_wait(barrier, n - 1)
    for g in range(groups):
        ship(0, g)

    for m in range(rows // LANES):
        block = dv[m * LANES:(m + 1) * LANES]
        eye = (lax.broadcasted_iota(jnp.int32, block.shape, 0) + m * LANES
               == lax.broadcasted_iota(jnp.int32, block.shape, 1))
        a_hi[m * LANES:(m + 1) * LANES], a_lo[m * LANES:(m + 1) * LANES] = split(
            jnp.where(eye, 0.0, -block))
    loads[2].wait()
    loads[3].wait()
    c_hi[...], c_lo[...] = split(-jnp.concatenate([lv[...], uv[...]], axis=0).T)

    for g in range(groups):
        d, sums = keep(xs[:, span(g)], 0, g)
        part[0, g:g + 1] = sums
        xs[:, span(g)] = d
        advance(g)

    def sweep(s, final):
        for g in range(groups):
            for side in range(2):
                @pl.when(has[side])
                def _():
                    copy(s - 1, side, g).wait_recv()
            for side in range(2):
                high, low = split(recv[s - 1, side, g])
                halo[side * width:(side + 1) * width, :LANES] = high
                halo[side * width:(side + 1) * width, LANES:] = low

            def rest(top, size):
                both = dot(c_hi[top:top + size], halo[...])
                cross = dot(c_lo[top:top + size], halo[:, :LANES])
                return acc[g, top:top + size] + (both[:, :LANES] + both[:, LANES:] + cross)

            total = jnp.zeros((1, LANES), jnp.float32)
            for top, size in ((0, width), (last, width), (width, last - width)):
                d, sums = keep(rest(top, size), top, g)
                total = total + sums
                if size == width and not final:
                    send[s, 1 if top == 0 else 0, g] = d
                    if top == last:
                        ship(s, g)
                xs[top:top + size, span(g)] += d
            part[s, g:g + 1] = total
            if final:
                pltpu.make_async_copy(
                    xs.at[:, span(g)], x_out.at[:, span(g)], out_sem.at[g]).start()
            else:
                advance(g)

    def body(s, carry):
        sweep(s, False)
        return carry

    inner = nears.shape[0]
    outer = n // inner
    seat, bench = lax.rem(me, inner), lax.div(me, inner)
    done = SWEEPS - 1

    def near(o):
        return pltpu.make_async_remote_copy(
            src_ref=part.at[:done], dst_ref=nears.at[seat],
            send_sem=psend.at[0, o], recv_sem=precv.at[0, o],
            device_id={"row": bench * inner + lax.rem(seat + o, inner)})

    def far(o):
        return pltpu.make_async_remote_copy(
            src_ref=fars.at[bench], dst_ref=fars.at[bench],
            send_sem=psend.at[1, o], recv_sem=precv.at[1, o],
            device_id={"row": lax.rem(bench + o, outer) * inner + seat})

    def late(o):
        return pltpu.make_async_remote_copy(
            src_ref=part.at[done], dst_ref=lates.at[me],
            send_sem=psend.at[2, o], recv_sem=precv.at[2, o],
            device_id={"row": lax.rem(me + o, n)})

    def over(count, action):
        def one(o, carry):
            action(o)
            return carry

        lax.fori_loop(1, count, one, 0)

    lax.fori_loop(1, SWEEPS - 1, body, 0)
    over(inner, lambda o: near(o).start())
    nears[seat] = part[:done]
    sweep(SWEEPS - 1, True)
    over(n, lambda o: late(o).start())
    lates[me] = part[done]
    over(inner, lambda o: near(o).wait_recv())
    sums = nears[0]
    for j in range(1, inner):
        sums = sums + nears[j]
    fars[bench] = sums
    over(outer, lambda o: far(o).start())

    def drain(s, carry):
        for side in range(2):
            for g in range(groups):
                @pl.when(has[1 - side])
                def _():
                    copy(s, side, g).wait_send()
        return carry

    lax.fori_loop(0, SWEEPS - 1, drain, 0)
    over(inner, lambda o: near(o).wait_send())
    over(outer, lambda o: far(o).wait_recv())
    norms = fars[0]
    for j in range(1, outer):
        norms = norms + fars[j]
    norms = jnp.sqrt(norms)
    for s in range(done):
        for g in range(groups):
            norm_out[s:s + 1, span(g)] = norms[s, g:g + 1]
    over(n, lambda o: late(o).wait_recv())
    norm = jnp.sqrt(lax.fori_loop(1, n, lambda j, t: t + lates[j], lates[0]))
    for g in range(groups):
        norm_out[done:, span(g)] = norm[g:g + 1]
    over(outer, lambda o: far(o).wait_send())
    over(n, lambda o: late(o).wait_send())
    for g in range(groups):
        pltpu.make_async_copy(xs.at[:, span(g)], x_out.at[:, span(g)], out_sem.at[g]).wait()


def local(n, diag_blocks, lower_coupling, upper_coupling, right_sides):
    rows, cols = right_sides.shape
    width = lower_coupling.shape[1]
    groups = cols // LANES
    inner = max(a for a in range(1, n + 1) if n % a == 0 and a * a <= n)
    f32, bf16 = jnp.float32, jnp.bfloat16
    return pl.pallas_call(
        functools.partial(kernel, n),
        out_shape=(jax.ShapeDtypeStruct((rows, cols), f32), jax.ShapeDtypeStruct((SWEEPS, cols), f32)),
        in_specs=[pl.BlockSpec(memory_space=pl.ANY)] * 4,
        out_specs=(pl.BlockSpec(memory_space=pl.ANY), pl.BlockSpec(memory_space=pltpu.VMEM)),
        scratch_shapes=[
            pltpu.VMEM((rows, rows), f32),
            pltpu.VMEM((width, rows), f32),
            pltpu.VMEM((width, rows), f32),
            pltpu.VMEM((rows, cols), f32),
            pltpu.VMEM((rows, rows), bf16),
            pltpu.VMEM((rows, rows), bf16),
            pltpu.VMEM((rows, 2 * width), bf16),
            pltpu.VMEM((rows, 2 * width), bf16),
            pltpu.VMEM((rows, LANES), f32),
            pltpu.VMEM((groups, rows, LANES), f32),
            pltpu.VMEM((rows, 2 * LANES), bf16),
            pltpu.VMEM((2 * width, 2 * LANES), bf16),
            pltpu.VMEM((SWEEPS - 1, 2, groups, width, LANES), f32),
            pltpu.VMEM((SWEEPS - 1, 2, groups, width, LANES), f32),
            pltpu.VMEM((SWEEPS, groups, LANES), f32),
            pltpu.VMEM((inner, SWEEPS - 1, groups, LANES), f32),
            pltpu.VMEM((n // inner, SWEEPS - 1, groups, LANES), f32),
            pltpu.VMEM((n, groups, LANES), f32),
            pltpu.SemaphoreType.DMA((4,)),
            pltpu.SemaphoreType.DMA((SWEEPS - 1, 2, groups)),
            pltpu.SemaphoreType.DMA((SWEEPS - 1, 2, groups)),
            pltpu.SemaphoreType.DMA((3, n)),
            pltpu.SemaphoreType.DMA((3, n)),
            pltpu.SemaphoreType.DMA((groups,)),
        ],
        compiler_params=pltpu.CompilerParams(
            collective_id=0, has_side_effects=True),
    )(diag_blocks, lower_coupling.T, upper_coupling.T, right_sides)


def solution(mesh):
    return jax.shard_map(
        functools.partial(local, mesh.shape["row"]),
        mesh=mesh,
        in_specs=(P("row", None), P("row", None), P("row", None), P("row", "grp")),
        out_specs=(P("row", "grp"), P(None, "grp")),
        check_vma=False,
    )
```

```python
import functools

import jax
import jax.numpy as jnp
from jax import lax
from jax.experimental import pallas as pl
from jax.experimental.pallas import tpu as pltpu
from jax.sharding import PartitionSpec as P

SWEEPS = 8
LANES = 128


def split(value):
    high = value.astype(jnp.bfloat16)
    low = (value - high.astype(jnp.float32)).astype(jnp.bfloat16)
    return high, low


def dot(left, right):
    return jnp.dot(left, right, preferred_element_type=jnp.float32)


def kernel(
    n, d_hbm, l_hbm, u_hbm, b_hbm, x_out, norm_out,
    dv, lv, uv, xs, a_hi, a_lo, c_hi, c_lo, inv, acc, rhs, halo,
    send, recv, part, nears, fars, lates, load_sem, send_sem, recv_sem, psend, precv,
):
    me = lax.axis_index("row")
    rows, cols = xs.shape
    width = lv.shape[0]
    groups = cols // LANES
    has = (me > 0, me < n - 1)
    last = rows - width

    loads = [pltpu.make_async_copy(d_hbm, dv, load_sem.at[0]),
             pltpu.make_async_copy(b_hbm, xs, load_sem.at[1]),
             pltpu.make_async_copy(l_hbm, lv, load_sem.at[2]),
             pltpu.make_async_copy(u_hbm, uv, load_sem.at[3])]
    for load in loads:
        load.start()

    barrier = pltpu.get_barrier_semaphore()

    def greet(o, carry):
        pl.semaphore_signal(barrier, inc=1, device_id={"row": lax.rem(me + o, n)})
        return carry

    lax.fori_loop(1, n, greet, 0)

    for side in range(2):
        @pl.when(jnp.logical_not(has[side]))
        def _():
            recv[:, side] = jnp.zeros_like(recv[:, side])

    def copy(s, side, g):
        target = me + 1 if side == 0 else me - 1
        return pltpu.make_async_remote_copy(
            src_ref=send.at[s, side, g], dst_ref=recv.at[s, side, g],
            send_sem=send_sem.at[s, side, g], recv_sem=recv_sem.at[s, side, g],
            device_id={"row": target})

    def ship(s, g):
        for side in range(2):
            @pl.when(has[1 - side])
            def _():
                copy(s, side, g).start()

    def keep(r, top, g):
        size = r.shape[0]
        d = r * inv[top:top + size]
        high, low = split(d)
        rhs[top:top + size, :LANES] = high
        rhs[top:top + size, LANES:] = low
        return d, jnp.sum(r * r, axis=0, keepdims=True)

    def advance(g):
        both = dot(a_hi[...], rhs[...])
        acc[g] = both[:, :LANES] + both[:, LANES:] + dot(a_lo[...], rhs[:, :LANES])

    def span(g):
        return slice(g * LANES, (g + 1) * LANES)

    loads[0].wait()
    for m in range(rows // LANES):
        block = dv[m * LANES:(m + 1) * LANES, m * LANES:(m + 1) * LANES]
        eye = (lax.broadcasted_iota(jnp.int32, block.shape, 0)
               == lax.broadcasted_iota(jnp.int32, block.shape, 1))
        pivot = jnp.sum(jnp.where(eye, block, 0.0), axis=1, keepdims=True)
        inv[m * LANES:(m + 1) * LANES] = jnp.broadcast_to(1.0 / pivot, block.shape)
    loads[1].wait()
    for g in range(groups):
        send[0, 1, g] = xs[:width, span(g)] * inv[:width]
        send[0, 0, g] = xs[last:, span(g)] * inv[last:]
    pl.semaphore_wait(barrier, n - 1)
    for g in range(groups):
        ship(0, g)

    for m in range(rows // LANES):
        block = dv[m * LANES:(m + 1) * LANES]
        eye = (lax.broadcasted_iota(jnp.int32, block.shape, 0) + m * LANES
               == lax.broadcasted_iota(jnp.int32, block.shape, 1))
        a_hi[m * LANES:(m + 1) * LANES], a_lo[m * LANES:(m + 1) * LANES] = split(
            jnp.where(eye, 0.0, -block))
    loads[2].wait()
    loads[3].wait()
    c_hi[...], c_lo[...] = split(-jnp.concatenate([lv[...], uv[...]], axis=0).T)

    for g in range(groups):
        d, sums = keep(xs[:, span(g)], 0, g)
        part[0, g:g + 1] = sums
        xs[:, span(g)] = d
        advance(g)

    def sweep(s, final):
        for g in range(groups):
            for side in range(2):
                @pl.when(has[side])
                def _():
                    copy(s - 1, side, g).wait_recv()
            for side in range(2):
                high, low = split(recv[s - 1, side, g])
                halo[side * width:(side + 1) * width, :LANES] = high
                halo[side * width:(side + 1) * width, LANES:] = low

            def rest(top, size):
                both = dot(c_hi[top:top + size], halo[...])
                cross = dot(c_lo[top:top + size], halo[:, :LANES])
                return acc[g, top:top + size] + (both[:, :LANES] + both[:, LANES:] + cross)

            total = jnp.zeros((1, LANES), jnp.float32)
            for top, size in ((0, width), (last, width), (width, last - width)):
                d, sums = keep(rest(top, size), top, g)
                total = total + sums
                if size == width and not final:
                    send[s, 1 if top == 0 else 0, g] = d
                    if top == last:
                        ship(s, g)
                if final:
                    x_out[top:top + size, span(g)] = xs[top:top + size, span(g)] + d
                else:
                    xs[top:top + size, span(g)] += d
            part[s, g:g + 1] = total
            if not final:
                advance(g)

    def body(s, carry):
        sweep(s, False)
        return carry

    inner = nears.shape[0]
    outer = n // inner
    seat, bench = lax.rem(me, inner), lax.div(me, inner)
    done = SWEEPS - 1

    def near(o):
        return pltpu.make_async_remote_copy(
            src_ref=part.at[:done], dst_ref=nears.at[seat],
            send_sem=psend.at[0, o], recv_sem=precv.at[0, o],
            device_id={"row": bench * inner + lax.rem(seat + o, inner)})

    def far(o):
        return pltpu.make_async_remote_copy(
            src_ref=fars.at[bench], dst_ref=fars.at[bench],
            send_sem=psend.at[1, o], recv_sem=precv.at[1, o],
            device_id={"row": lax.rem(bench + o, outer) * inner + seat})

    def late(o):
        return pltpu.make_async_remote_copy(
            src_ref=part.at[done], dst_ref=lates.at[me],
            send_sem=psend.at[2, o], recv_sem=precv.at[2, o],
            device_id={"row": lax.rem(me + o, n)})

    def over(count, action):
        def one(o, carry):
            action(o)
            return carry

        lax.fori_loop(1, count, one, 0)

    lax.fori_loop(1, SWEEPS - 1, body, 0)
    over(inner, lambda o: near(o).start())
    nears[seat] = part[:done]
    sweep(SWEEPS - 1, True)
    over(n, lambda o: late(o).start())
    lates[me] = part[done]
    over(inner, lambda o: near(o).wait_recv())
    sums = nears[0]
    for j in range(1, inner):
        sums = sums + nears[j]
    fars[bench] = sums
    over(outer, lambda o: far(o).start())

    def drain(s, carry):
        for side in range(2):
            for g in range(groups):
                @pl.when(has[1 - side])
                def _():
                    copy(s, side, g).wait_send()
        return carry

    lax.fori_loop(0, SWEEPS - 1, drain, 0)
    over(inner, lambda o: near(o).wait_send())
    over(outer, lambda o: far(o).wait_recv())
    norms = fars[0]
    for j in range(1, outer):
        norms = norms + fars[j]
    norms = jnp.sqrt(norms)
    for s in range(done):
        for g in range(groups):
            norm_out[s:s + 1, span(g)] = norms[s, g:g + 1]
    over(n, lambda o: late(o).wait_recv())
    norm = jnp.sqrt(lax.fori_loop(1, n, lambda j, t: t + lates[j], lates[0]))
    for g in range(groups):
        norm_out[done:, span(g)] = norm[g:g + 1]
    over(outer, lambda o: far(o).wait_send())
    over(n, lambda o: late(o).wait_send())


def local(n, diag_blocks, lower_coupling, upper_coupling, right_sides):
    rows, cols = right_sides.shape
    width = lower_coupling.shape[1]
    groups = cols // LANES
    inner = max(a for a in range(1, n + 1) if n % a == 0 and a * a <= n)
    f32, bf16 = jnp.float32, jnp.bfloat16
    return pl.pallas_call(
        functools.partial(kernel, n),
        out_shape=(pltpu.VMEM((rows, cols), f32), pltpu.VMEM((SWEEPS, cols), f32)),
        in_specs=[pl.BlockSpec(memory_space=pltpu.HBM)] * 4,
        out_specs=[pl.BlockSpec(memory_space=pltpu.VMEM)] * 2,
        scratch_shapes=[
            pltpu.VMEM((rows, rows), f32),
            pltpu.VMEM((width, rows), f32),
            pltpu.VMEM((width, rows), f32),
            pltpu.VMEM((rows, cols), f32),
            pltpu.VMEM((rows, rows), bf16),
            pltpu.VMEM((rows, rows), bf16),
            pltpu.VMEM((rows, 2 * width), bf16),
            pltpu.VMEM((rows, 2 * width), bf16),
            pltpu.VMEM((rows, LANES), f32),
            pltpu.VMEM((groups, rows, LANES), f32),
            pltpu.VMEM((rows, 2 * LANES), bf16),
            pltpu.VMEM((2 * width, 2 * LANES), bf16),
            pltpu.VMEM((SWEEPS - 1, 2, groups, width, LANES), f32),
            pltpu.VMEM((SWEEPS - 1, 2, groups, width, LANES), f32),
            pltpu.VMEM((SWEEPS, groups, LANES), f32),
            pltpu.VMEM((inner, SWEEPS - 1, groups, LANES), f32),
            pltpu.VMEM((n // inner, SWEEPS - 1, groups, LANES), f32),
            pltpu.VMEM((n, groups, LANES), f32),
            pltpu.SemaphoreType.DMA((4,)),
            pltpu.SemaphoreType.DMA((SWEEPS - 1, 2, groups)),
            pltpu.SemaphoreType.DMA((SWEEPS - 1, 2, groups)),
            pltpu.SemaphoreType.DMA((3, n)),
            pltpu.SemaphoreType.DMA((3, n)),
        ],
        compiler_params=pltpu.CompilerParams(
            collective_id=0, has_side_effects=True, vmem_limit_bytes=62 * 2**20),
    )(diag_blocks, lower_coupling.T, upper_coupling.T, right_sides)


def solution(mesh):
    return jax.shard_map(
        functools.partial(local, mesh.shape["row"]),
        mesh=mesh,
        in_specs=(P("row", None), P("row", None), P("row", None), P("row", "grp")),
        out_specs=(P("row", "grp"), P(None, "grp")),
        check_vma=False,
    )
```
